32 devices in a mesh: runs: 2 (over x), space: 16 (over z, y, core).
Axes of the slice: x: 2, y: 2, z: 4, core: 2. Of those that a mesh axis runs over, the one named last changes fastest.
Arguments:
- levels: float32 [4, 24, 32, 16, 128], P('runs', None, 'space'), parts along dimension 0, may hold values from -6 to 6
- region_offset: int32 [6], P('runs'), parts along dimension 0, may hold values from 0 to 127, as said below
- advect: float32 [3, 24, 24], replicated, may hold values from -1 to 1
- coupling: float32 [24, 24], replicated, may hold values from -0.8 to 0.8
- diffusion: float32 [24], replicated, may hold values from 0.02 to 0.15
Outputs:
- levels_out: float32 [4, 24, 32, 16, 128], P('runs', None, 'space'), parts along dimension 0
The draws below stay inside these ranges and needn't reach their ends.
There are 2 independent parts, one for each index of `runs`. The reference program is written for one: setup_inputs(seed, part) draws one part's arguments, and reference() takes and returns one part's arrays. A program takes and returns all parts, laid end to end along the dimension named above; an argument that names none is the same for every part. Nothing has to cross between parts.
Inputs may be any that keep to these rules, and one draw needn't show every extreme that they name: `region_offset`: the first entry lies in 0 to 31, the second in 0 to 15, the third in 0 to 127; the refined box may wrap around the periodic coarse grid.
All inputs are finite; a program needn't handle non-finite values.
Results may differ from the reference program's by a relative error of at most 0.0001.
Values sent between devices are 32-bit elements; how exact they have to be, the bound alone decides.
A program may use at most 128 MiB of HBM per device.

```python
import math
import jax
import jax.numpy as jnp
from jax import lax

FIELDS = 24
LEVELS = 2
NY = 16
NZ = 128
NX = 32


def draw_region_offset(key, part):
    subkeys = jax.random.split(jax.random.fold_in(key, 7), 3)
    across = jax.random.randint(subkeys[0], (1,), 0, NX)
    rows_start = jax.random.randint(subkeys[1], (1,), 0, NY)
    depth_start = jax.random.randint(subkeys[2], (1,), 0, NZ)
    return jnp.concatenate([across, rows_start, depth_start]).astype(jnp.int32)


def shard_levels(stream_key, extent, shards, low, high):
    def one(dim, blocks):
        draws = jax.random.uniform(jax.random.fold_in(jax.random.fold_in(stream_key, 6), dim), (blocks,), jnp.float32, low / len(shards), high / len(shards))
        return jnp.repeat(jnp.exp(draws), extent[dim] // blocks).reshape((-1,) + (1,) * (len(extent) - dim - 1))

    gain = one(*shards[0])
    for cut in shards[1:]:
        gain = gain * one(*cut)
    return gain


def scatter_about(own_key, extent, width, bound, cuts=(), dtype=jnp.bfloat16):
    gain = shard_levels(own_key, extent, cuts, -0.22, 0.18) if cuts else 1.0
    result = jax.random.normal(own_key, extent, jnp.float32) * width * gain
    return jnp.minimum(jnp.maximum(result, -bound), bound).astype(dtype)


def setup_inputs(seed: int = 0, part: int = 0) -> dict:
    key_of = jax.random.split(jax.random.key(seed), 6)
    part_keys = jax.random.split(jax.random.fold_in(key_of[5], part), 6)
    levels = scatter_about(part_keys[0], (LEVELS, FIELDS, NX, NY, NZ), 1.0, 6.0, ((2, 16),), jnp.float32)
    region_offset = draw_region_offset(jax.random.fold_in(jax.random.fold_in(key_of[5], part), 71), part)
    advect = scatter_about(key_of[2], (3, FIELDS, FIELDS), 0.25, 1.0, (), jnp.float32)
    coupling = scatter_about(key_of[3], (FIELDS, FIELDS), 0.2, 0.8, (), jnp.float32)
    diffusion = jnp.clip(jnp.exp(jax.random.uniform(key_of[4], (FIELDS,), jnp.float32, math.log(0.02), math.log(0.15))), 0.02, 0.15)
    return {"levels": levels, "region_offset": region_offset, "advect": advect, "coupling": coupling, "diffusion": diffusion}


coarse_step = 0.25
coarse_spacing = 1.0
damping = 0.2
fractions = (0.0, 0.5, 0.5, 1.0)
highest = lax.Precision.HIGHEST


def stencil_terms(padded, dimension, length, spacing):
    shifted = [lax.slice_in_dim(padded, k, k + length, axis=dimension) for k in range(5)]
    gradient = (shifted[0] - 8.0 * shifted[1] + 8.0 * shifted[3] - shifted[4]) / (12.0 * spacing)
    second = (16.0 * (shifted[1] + shifted[3]) - shifted[0] - shifted[4] - 30.0 * shifted[2]) / (12.0 * spacing * spacing)
    fourth = shifted[0] + shifted[4] - 4.0 * (shifted[1] + shifted[3]) + 6.0 * shifted[2]
    return gradient, second, fourth


def tendency(fields, padded, spacing, mixing, diffusion):
    stencils = [stencil_terms(padded[d - 1], d, fields.shape[d], spacing) for d in (1, 2, 3)]
    stacked = jnp.concatenate([stencils[0][0], stencils[1][0], stencils[2][0], fields], axis=0)
    coupled = jnp.einsum("fg,gxyz->fxyz", mixing, stacked, precision=highest)
    second = stencils[0][1] + stencils[1][1] + stencils[2][1]
    fourth = stencils[0][2] + stencils[1][2] + stencils[2][2]
    return coupled + diffusion[:, None, None, None] * second - (damping / (16.0 * spacing)) * fourth


def advance(fields, timestep, evaluate):
    rate_one = evaluate(fields, 0)
    rate_two = evaluate(fields + (0.5 * timestep) * rate_one, 1)
    rate_three = evaluate(fields + (0.5 * timestep) * rate_two, 2)
    rate_four = evaluate(fields + timestep * rate_three, 3)
    return fields + (timestep / 6.0) * (rate_one + 2.0 * rate_two + 2.0 * rate_three + rate_four)


def mixing_matrix(advect, coupling):
    symmetric = 0.5 * (advect + jnp.swapaxes(advect, 1, 2))
    return jnp.concatenate([symmetric[0], symmetric[1], symmetric[2], coupling], axis=1)


def hat_weights(fine_index, coarse_index):
    location = 0.5 * fine_index.astype(jnp.float32)[:, None] + 0.75
    return jnp.maximum(0.0, 1.0 - jnp.abs(location - coarse_index.astype(jnp.float32)[None, :]))


def wrap_pad(fields, dimension):
    length = fields.shape[dimension]
    low_rim = lax.slice_in_dim(fields, length - 2, length, axis=dimension)
    high_rim = lax.slice_in_dim(fields, 0, 2, axis=dimension)
    return jnp.concatenate([low_rim, fields, high_rim], axis=dimension)


def with_ghosts(fields, ghost, dimension):
    return jnp.concatenate([lax.slice_in_dim(ghost, 0, 2, axis=dimension), fields, lax.slice_in_dim(ghost, 2, 4, axis=dimension)], axis=dimension)


def prolong(weights_across, weights_rows, weights_depth, source):
    return jnp.einsum("ai,bj,ck,fijk->fabc", weights_across, weights_rows, weights_depth, source, precision=highest)


def window_of(parent, region_offset):
    rolled = jnp.roll(parent, (2 - region_offset[0], 2 - region_offset[1], 2 - region_offset[2]), axis=(1, 2, 3))
    return rolled[:, : NX // 2 + 4, : NY // 2 + 4, : NZ // 2 + 4]


def ghost_layers(window):
    counts = (NX, NY, NZ)
    interior = [hat_weights(jnp.arange(2, n + 2), jnp.arange(n // 2 + 4)) for n in counts]
    exterior = [hat_weights(jnp.concatenate([jnp.arange(2), n + 2 + jnp.arange(2)]), jnp.arange(n // 2 + 4)) for n in counts]
    return (prolong(exterior[0], interior[1], interior[2], window),
            prolong(interior[0], exterior[1], interior[2], window),
            prolong(interior[0], interior[1], exterior[2], window))


def reference(levels, region_offset, advect, coupling, diffusion):
    mixing = mixing_matrix(advect, coupling)
    coarse_level = levels[0]
    fine_level = levels[1]

    def coarse_rate(fields, section_index):
        padded = [wrap_pad(fields, d) for d in (1, 2, 3)]
        return tendency(fields, padded, coarse_spacing, mixing, diffusion)

    coarse_new = advance(coarse_level, coarse_step, coarse_rate)
    ghosts_old = ghost_layers(window_of(coarse_level, region_offset))
    ghosts_new = ghost_layers(window_of(coarse_new, region_offset))

    def fine_rate(fields, section_index, substep):
        weight = (substep + fractions[section_index]) * 0.5
        ghosts = [(1.0 - weight) * before_step + weight * after_step for before_step, after_step in zip(ghosts_old, ghosts_new)]
        padded = [with_ghosts(fields, ghosts[d - 1], d) for d in (1, 2, 3)]
        return tendency(fields, padded, 0.5 * coarse_spacing, mixing, diffusion)

    for substep in range(2):
        fine_level = advance(fine_level, 0.5 * coarse_step, lambda fields, section_index: fine_rate(fields, section_index, substep))

    restricted = fine_level.reshape(FIELDS, NX // 2, 2, NY // 2, 2, NZ // 2, 2).mean(axis=(2, 4, 6))
    rolled = jnp.roll(coarse_new, (-region_offset[0], -region_offset[1], -region_offset[2]), axis=(1, 2, 3))
    rolled = rolled.at[:, : NX // 2, : NY // 2, : NZ // 2].set(restricted)
    coarse_final = jnp.roll(rolled, (region_offset[0], region_offset[1], region_offset[2]), axis=(1, 2, 3))
    return jnp.stack([coarse_final, fine_level])
```

```python
import jax
import jax.numpy as jnp
from jax import lax
from jax.experimental import pallas as pl
from jax.experimental.pallas import tpu as pltpu
from jax.sharding import PartitionSpec as P

coarse_step = 0.25
damping = 0.2
fractions = (0.0, 0.5, 0.5, 1.0)
f32, bf16 = jnp.float32, jnp.bfloat16


def split_dot(x, m):
    hi = x.astype(bf16)
    lo = (x - hi.astype(f32)).astype(bf16)
    return jnp.dot(hi, m, preferred_element_type=f32) + jnp.dot(lo, m, preferred_element_type=f32)


def hat(j):
    location = 2 * j + 3
    low = location // 4
    return low, 1.0 - (location % 4) / 4.0, (location % 4) / 4.0


def kernel(n, off_ref, mix_ref, diff_ref, lev_ref, zsel_ref, exp_ref, expx_ref, mean_ref, place_ref, out_ref,
           u_buf, l_buf, r_buf, start, acc, weights, pay, gath, gy, gz, gx, means, landed,
           halo_send, halo_recv, all_send, all_recv):
    planes, rows, fields, depth = lev_ref.shape[1:]
    total = planes * n
    half_x, half_y, half_z = total // 2, rows // 2, depth // 2
    win_y = half_y + 4
    me = lax.axis_index("space")
    right, left = lax.rem(me + 1, n), lax.rem(me + n - 1, n)
    p, q = off_ref[0], off_ref[1]

    barrier = pltpu.get_barrier_semaphore()

    @pl.loop(1, n)
    def _(k):
        pl.semaphore_signal(barrier, inc=1, device_id={"space": lax.rem(me + k, n)}, device_id_type=pl.DeviceIdType.MESH)

    pl.semaphore_wait(barrier, n - 1)

    def send_all(src, dst, kind):
        @pl.loop(1, n)
        def _(k):
            pltpu.make_async_remote_copy(
                src_ref=src, dst_ref=dst, send_sem=all_send.at[kind, k], recv_sem=all_recv.at[kind, k],
                device_id={"space": lax.rem(me + k, n)}, device_id_type=pl.DeviceIdType.MESH).start()

    def wait_all(src, dst, kind):
        @pl.loop(1, n)
        def _(k):
            pltpu.make_async_remote_copy(
                src_ref=src, dst_ref=dst, send_sem=all_send.at[kind, k], recv_sem=all_recv.at[kind, k],
                device_id={"space": lax.rem(me + k, n)}, device_id_type=pl.DeviceIdType.MESH).wait()

    def halo(slot):
        copies = []
        for side, target, dst in ((0, right, l_buf), (1, left, r_buf)):
            copies.append(pltpu.make_async_remote_copy(
                src_ref=u_buf.at[slot, :, pl.ds(2, rows)], dst_ref=dst.at[slot],
                send_sem=halo_send.at[slot, side], recv_sem=halo_recv.at[slot, side],
                device_id={"space": target}, device_id_type=pl.DeviceIdType.MESH))
        return copies

    def pack_window(load, kind):
        for x in range(planes):
            picked = [load(x, lax.rem(q + rows - 2 + a, rows)) for a in range(win_y)]
            got = split_dot(jnp.concatenate(picked, axis=0), zsel_ref[...])
            for t in range(win_y // 2):
                even = got[2 * t * fields:(2 * t + 1) * fields, :depth]
                odd = got[(2 * t + 1) * fields:(2 * t + 2) * fields, :depth]
                pay[kind, x, t] = even + pltpu.roll(odd, half_z, 1)
            extra = got[:fields, depth:]
            for a in range(1, win_y):
                extra = extra + pltpu.roll(got[a * fields:(a + 1) * fields, depth:], 4 * a, 1)
            pay[kind, x, win_y // 2] = extra

    lanes = lax.broadcasted_iota(jnp.int32, (fields, depth), 1)
    stage = [0]

    def set_weights(spacing):
        column = lax.broadcasted_iota(jnp.int32, (fields, 4 * fields), 1)
        row = lax.broadcasted_iota(jnp.int32, (fields, 4 * fields), 0)
        c = damping / (16.0 * spacing)
        square = 12.0 * spacing * spacing
        diff = diff_ref[:, :1]
        diagonal = diff * (-90.0 / square) - 18.0 * c
        m = mix_ref[...]
        m = jnp.where(column < 3 * fields, m * (1.0 / (12.0 * spacing)),
                      m + jnp.where(column - 3 * fields == row, diagonal, 0.0))
        hi = m.astype(bf16).astype(f32)
        lo = m - hi
        weights[...] = jnp.concatenate(
            [jnp.concatenate([hi, hi], axis=1), jnp.concatenate([lo, jnp.zeros_like(lo)], axis=1)], axis=0).astype(bf16)
        dif = diff_ref[...]
        return dif * (16.0 / square) + 4.0 * c, dif * (-1.0 / square) - c

    def run_stage(section, step, near, far, t, last_store):
        slot = stage[0] % 2
        following = 1 - slot
        copies = halo(slot)
        for copy in copies:
            copy.start()
        if stage[0] > 0:
            for copy in halo(following):
                copy.wait_send()
        for copy in copies:
            copy.wait_recv()
        if t is not None:
            for edge, buf in ((0, l_buf), (n - 1, r_buf)):
                @pl.when(me == edge)
                def _(buf=buf):
                    @pl.loop(0, rows)
                    def _(y):
                        for x in range(planes):
                            buf[slot, x, y] = (1.0 - t) * gx[0, x, y] + t * gx[1, x, y]

        def body(y, carry):
            line = [l_buf[slot, 0, y], l_buf[slot, 1, y], u_buf[slot, 0, y + 2], u_buf[slot, 1, y + 2],
                    r_buf[slot, 0, y], r_buf[slot, 1, y]]
            stacks, even = [], []
            for x in range(planes):
                c = line[x + 2]
                terms = [(line[x], line[x + 1], line[x + 3], line[x + 4]),
                         tuple(u_buf[slot, x, y + 2 + k] for k in (-2, -1, 1, 2))]
                if t is None:
                    lo2 = lo1 = hi1 = hi2 = c
                else:
                    g = (1.0 - t) * gz[0, x, y] + t * gz[1, x, y]
                    lo2 = jnp.where(lanes >= depth - 2, g, c)
                    lo1 = jnp.where(lanes == depth - 1, g, c)
                    hi1 = jnp.where(lanes == 0, g, c)
                    hi2 = jnp.where(lanes <= 1, g, c)
                terms.append((pltpu.roll(lo2, 2, 1), pltpu.roll(lo1, 1, 1),
                              pltpu.roll(hi1, depth - 1, 1), pltpu.roll(hi2, depth - 2, 1)))
                stacks.append(jnp.concatenate(
                    [8.0 * (p1 - m1) - (p2 - m2) for m2, m1, p1, p2 in terms] + [c], axis=0))
                one = sum(m1 + p1 for _, m1, p1, _ in terms)
                two = sum(m2 + p2 for m2, _, _, p2 in terms)
                even.append(near * one + far * two)
            wide = jnp.concatenate(stacks, axis=1)
            hi = wide.astype(bf16)
            lo = (wide - hi.astype(f32)).astype(bf16)
            got = jnp.dot(weights[...], jnp.concatenate([hi, lo], axis=0), preferred_element_type=f32)
            got = got[:fields] + got[fields:]
            for x in range(planes):
                rate = got[:, x * depth:(x + 1) * depth] + even[x]
                if section == 0:
                    acc[x, y] = start[x, y] + (step / 6.0) * rate
                elif section < 3:
                    acc[x, y] = acc[x, y] + (step / 3.0) * rate
                if section < 3:
                    u_buf[following, x, y + 2] = start[x, y] + (step if section == 2 else 0.5 * step) * rate
                else:
                    last_store(x, y, acc[x, y] + (step / 6.0) * rate, following)
            return carry

        lax.fori_loop(0, rows, body, 0, unroll=2)
        stage[0] += 1

    def wrap_rows():
        slot = stage[0] % 2
        for x in range(planes):
            for k in range(2):
                u_buf[slot, x, k] = u_buf[slot, x, rows + k]
                u_buf[slot, x, rows + 2 + k] = u_buf[slot, x, 2 + k]

    def ghost_rows(t):
        slot = stage[0] % 2
        for x in range(planes):
            for k in range(4):
                row = k if k < 2 else rows + k
                u_buf[slot, x, row] = (1.0 - t) * gy[0, x, k] + t * gy[1, x, k]

    near, far = set_weights(1.0)

    @pl.loop(0, rows)
    def _(y):
        for x in range(planes):
            start[x, y] = lev_ref[0, x, y]
            u_buf[0, x, y + 2] = lev_ref[0, x, y]

    pack_window(lambda x, y: lev_ref[0, x, y], 0)
    gath[0, me] = pay[0]
    send_all(pay.at[0], gath.at[0, me], 0)

    def coarse_store(x, y, value, following):
        start[x, y] = value

    for section in range(4):
        wrap_rows()
        run_stage(section, coarse_step, near, far, None, coarse_store)

    pack_window(lambda x, y: start[x, y], 1)
    gath[1, me] = pay[1]
    send_all(pay.at[1], gath.at[1, me], 1)

    near, far = set_weights(0.5)

    @pl.loop(0, rows)
    def _(y):
        for x in range(planes):
            out_ref[0, x, y] = start[x, y]
            start[x, y] = lev_ref[1, x, y]
            u_buf[stage[0] % 2, x, y + 2] = lev_ref[1, x, y]

    wait_all(pay.at[0], gath.at[0, me], 0)
    wait_all(pay.at[1], gath.at[1, me], 1)

    def window_rows(t, first, w0, w1, which):
        g0 = lax.rem(p + total - 2 + first, total)
        g1 = lax.rem(p + total - 1 + first, total)
        tiles = [w0 * gath[t, g0 // planes, g0 % planes, k] + w1 * gath[t, g1 // planes, g1 % planes, k]
                 for k in range(win_y // 2 + 1)]
        main = split_dot(jnp.concatenate(tiles[:-1], axis=0), exp_ref[...])
        turned = [tiles[-1]] + [pltpu.roll(tiles[-1], depth - 4 * a, 1) for a in range(1, win_y)]
        extra = split_dot(jnp.concatenate(turned, axis=0), expx_ref[...])
        found = []
        for part in which:
            found.append([main[(a // 2) * fields:(a // 2 + 1) * fields,
                               (2 * part + a % 2) * depth:(2 * part + a % 2 + 1) * depth]
                          + extra[a * fields:(a + 1) * fields, part * depth:(part + 1) * depth] for a in range(win_y)])
        return found

    def mix_rows(lines, j):
        low, w0, w1 = hat(j)
        return w0 * lines[low] + w1 * lines[low + 1]

    @pl.loop(0, 2)
    def _(t):
        for x in range(planes):
            shift, w0, w1 = hat(x + 2)
            inner, outer = window_rows(t, me * (planes // 2) + shift, w0, w1, (0, 1))
            for k in range(4):
                gy[t, x, k] = mix_rows(inner, k if k < 2 else rows + k)
            for y in range(rows):
                gz[t, x, y] = mix_rows(outer, y + 2)
        for edge, base in ((0, 0), (n - 1, total + 2)):
            @pl.when(me == edge)
            def _(base=base):
                for x in range(2):
                    low, w0, w1 = hat(base + x)
                    inner, = window_rows(t, low, w0, w1, (0,))
                    for y in range(rows):
                        gx[t, x, y] = mix_rows(inner, y + 2)

    def fine_store(x, y, value, following):
        start[x, y] = value
        u_buf[following, x, y + 2] = value

    for substep in range(2):
        for section in range(4):
            t = 0.5 * (substep + fractions[section])
            ghost_rows(t)
            run_stage(section, 0.5 * coarse_step, near, far, t, fine_store)
    for copy in halo(1 - stage[0] % 2):
        copy.wait_send()

    folded = []
    for y in range(half_y):
        folded.append(start[0, 2 * y] + start[0, 2 * y + 1] + start[1, 2 * y] + start[1, 2 * y + 1])
    got = split_dot(jnp.concatenate(folded, axis=0), mean_ref[...])
    for t in range(half_y // 2):
        means[t] = (got[2 * t * fields:(2 * t + 1) * fields]
                    + pltpu.roll(got[(2 * t + 1) * fields:(2 * t + 2) * fields], half_z, 1))
        landed[me, t] = means[t]
    send_all(means, landed.at[me], 2)

    @pl.loop(0, rows)
    def _(y):
        for x in range(planes):
            out_ref[1, x, y] = start[x, y]

    wait_all(means, landed.at[me], 2)
    distance = lax.rem(lanes - off_ref[2] + depth, depth)
    for x in range(planes):
        relative = lax.rem(me * planes + x - p + total, total)
        source = lax.rem(relative, half_x)
        for k in range(half_y // 2):
            tile = landed[source, k]
            placed = split_dot(tile, place_ref[...])
            for parity in range(2):
                acc[0, 2 * k + parity] = placed[:, parity * depth:(parity + 1) * depth]
        for y in range(rows):
            row = lax.rem(y - q + rows, rows)
            value = acc[0, lax.rem(row, half_y)]
            limit = jnp.where(relative < half_x, jnp.where(row < half_y, half_z, 0), 0)
            out_ref[0, x, y] = jnp.where(distance < limit, value, out_ref[0, x, y])


def hats(fine, window):
    return jnp.maximum(0.0, 1.0 - jnp.abs(0.5 * fine.astype(f32) + 0.75 - window.astype(f32)))


def local(n, levels, region_offset, advect, coupling, diffusion):
    count, fields, planes, rows, depth = levels.shape
    half = depth // 2
    total = planes * n
    win_tiles = (rows // 2 + 4) // 2 + 1
    symmetric = 0.5 * (advect + jnp.swapaxes(advect, 1, 2))
    mixing = jnp.concatenate([symmetric[0], symmetric[1], symmetric[2], coupling], axis=1)
    spread = jnp.broadcast_to(diffusion[:, None], (fields, depth))
    swapped = jnp.transpose(levels, (0, 2, 3, 1, 4))
    r = region_offset[2]
    z = jnp.arange(depth, dtype=jnp.int32)[:, None]
    lane = jnp.arange(depth, dtype=jnp.int32)[None, :]
    zsel = jnp.concatenate([
        (lane < half) & (z == jnp.mod(r - 2 + lane, depth)),
        (lane < 4) & (z == jnp.mod(r - 2 + half + lane, depth))], axis=1).astype(bf16)
    outer = jnp.where(lane >= depth - 2, lane - (depth - 2), depth + 2 + lane)
    has = ((lane >= depth - 2) | (lane < 2)).astype(f32)
    parts = []
    for fine, mask in ((lane + 2, 1.0), (outer, has)):
        parts += [jnp.where(z < half, hats(fine, z), 0.0) * mask, jnp.where(z >= half, hats(fine, z - half), 0.0) * mask]
    expand = jnp.concatenate(parts, axis=1).astype(bf16)
    expandx = jnp.concatenate(
        [jnp.where(z < 4, hats(fine, z + half), 0.0) * mask for fine, mask in ((lane + 2, 1.0), (outer, has))],
        axis=1).astype(bf16)
    mean = ((z // 2 == lane) * 0.125).astype(bf16)
    target = jnp.mod(lane - r, depth)
    place = jnp.concatenate([(z == target) & (target < half), (z == target + half) & (target < half)], axis=1).astype(bf16)
    block = (planes, rows, fields, depth)
    vmem = pl.BlockSpec(memory_space=pltpu.VMEM)
    out = pl.pallas_call(
        lambda *refs: kernel(n, *refs),
        out_shape=jax.ShapeDtypeStruct(swapped.shape, f32),
        in_specs=[pl.BlockSpec(memory_space=pltpu.SMEM)] + [vmem] * 8,
        out_specs=vmem,
        scratch_shapes=[
            pltpu.VMEM((2, planes, rows + 4, fields, depth), f32),
            pltpu.VMEM((2,) + block, f32),
            pltpu.VMEM((2,) + block, f32),
            pltpu.VMEM(block, f32),
            pltpu.VMEM(block, f32),
            pltpu.VMEM((2 * fields, 8 * fields), bf16),
            pltpu.VMEM((2, planes, win_tiles, fields, depth), f32),
            pltpu.VMEM((2, n, planes, win_tiles, fields, depth), f32),
            pltpu.VMEM((2, planes, 4, fields, depth), f32),
            pltpu.VMEM((2,) + block, f32),
            pltpu.VMEM((2,) + block, f32),
            pltpu.VMEM((rows // 4, fields, depth), f32),
            pltpu.VMEM((n, rows // 4, fields, depth), f32),
            pltpu.SemaphoreType.DMA((2, 2)),
            pltpu.SemaphoreType.DMA((2, 2)),
            pltpu.SemaphoreType.DMA((3, n)),
            pltpu.SemaphoreType.DMA((3, n)),
        ],
        compiler_params=pltpu.CompilerParams(
            collective_id=0, has_side_effects=True, vmem_limit_bytes=48 * 1024 * 1024),
    )(region_offset, mixing, spread, swapped, zsel, expand, expandx, mean, place)
    return jnp.transpose(out, (0, 3, 1, 2, 4))


def solution(mesh):
    n = mesh.shape["space"]
    return jax.shard_map(
        lambda *args: local(n, *args),
        mesh=mesh,
        in_specs=(P("runs", None, "space", None, None), P("runs"), P(), P(), P()),
        out_specs=P("runs", None, "space", None, None),
        check_vma=False,
    )
```

```python
import jax
import jax.numpy as jnp
from jax import lax
from jax.experimental import pallas as pl
from jax.experimental.pallas import tpu as pltpu
from jax.sharding import PartitionSpec as P

coarse_step = 0.25
damping = 0.2
fractions = (0.0, 0.5, 0.5, 1.0)
f32, bf16 = jnp.float32, jnp.bfloat16


def split_dot(x, m):
    hi = x.astype(bf16)
    lo = (x - hi.astype(f32)).astype(bf16)
    return jnp.dot(hi, m, preferred_element_type=f32) + jnp.dot(lo, m, preferred_element_type=f32)


def hat(j):
    location = 2 * j + 3
    low = location // 4
    return low, 1.0 - (location % 4) / 4.0, (location % 4) / 4.0


def kernel(n, off_ref, mix_ref, diff_ref, lev_ref, zsel_ref, exp_ref, expx_ref, mean_ref, place_ref, out_ref,
           u_buf, l_buf, r_buf, start, acc, part, weights, weights_x, pay, gath_old, gath_new, gy, gz, gx, sums, landed,
           halo_send, halo_recv, all_send, all_recv):
    planes, rows, fields, depth = lev_ref.shape[1:]
    total = planes * n
    half_x, half_y, half_z = total // 2, rows // 2, depth // 2
    win_y = half_y + 4
    me = lax.axis_index("space")
    right, left = lax.rem(me + 1, n), lax.rem(me + n - 1, n)
    p, q = off_ref[0], off_ref[1]

    barrier = pltpu.get_barrier_semaphore()

    @pl.loop(1, n)
    def _(k):
        pl.semaphore_signal(barrier, inc=1, device_id={"space": lax.rem(me + k, n)}, device_id_type=pl.DeviceIdType.MESH)

    pl.semaphore_wait(barrier, n - 1)

    core = lax.rem(me, 2)
    pair = me // 2
    across = me + 2 - 4 * lax.rem(pair, 2)
    groups = n // 4
    first = pair - lax.rem(pair, 2)

    def remote(src, dst, kind, k, target):
        return pltpu.make_async_remote_copy(
            src_ref=src, dst_ref=dst, send_sem=all_send.at[kind, k], recv_sem=all_recv.at[kind, k],
            device_id={"space": target}, device_id_type=pl.DeviceIdType.MESH)

    def gather_start(dst, own, kind):
        remote(own, dst.at[core, pair], kind, 0, across).start()

    def gather_middle(dst, own, kind):
        remote(own, dst.at[core, pair], kind, 0, across).wait()

        @pl.loop(1, groups)
        def _(k):
            block = dst.at[core, pl.ds(first, 2)]
            remote(block, block, kind, k, lax.rem(me + 4 * k, n)).start()

    def gather_last(dst, kind):
        @pl.loop(1, groups)
        def _(k):
            block = dst.at[core, pl.ds(first, 2)]
            remote(block, block, kind, k, lax.rem(me + 4 * k, n)).wait()

        remote(dst.at[core], dst.at[core], kind, groups, me + 1 - 2 * core).start()

    def gather_end(dst, kind):
        remote(dst.at[core], dst.at[core], kind, groups, me + 1 - 2 * core).wait()

    def halo(slot):
        copies = []
        for side, target, dst in ((0, right, l_buf), (1, left, r_buf)):
            copies.append(pltpu.make_async_remote_copy(
                src_ref=u_buf.at[slot, :, pl.ds(2, rows)], dst_ref=dst.at[slot],
                send_sem=halo_send.at[slot, side], recv_sem=halo_recv.at[slot, side],
                device_id={"space": target}, device_id_type=pl.DeviceIdType.MESH))
        return copies

    def pack_window(load, kind):
        for x in range(planes):
            picked = [load(x, lax.rem(q + rows - 2 + a, rows)) for a in range(win_y)]
            got = split_dot(jnp.concatenate(picked, axis=0), zsel_ref[...])
            for t in range(win_y // 2):
                even = got[2 * t * fields:(2 * t + 1) * fields, :depth]
                odd = got[(2 * t + 1) * fields:(2 * t + 2) * fields, :depth]
                pay[kind, x, t] = even + pltpu.roll(odd, half_z, 1)
            extra = got[:fields, depth:]
            for a in range(1, win_y):
                extra = extra + pltpu.roll(got[a * fields:(a + 1) * fields, depth:], 4 * a, 1)
            pay[kind, x, win_y // 2] = extra

    def blend(load, t):
        if t in (0.0, 1.0):
            return load(int(t))
        return (1.0 - t) * load(0) + t * load(1)

    lanes = lax.broadcasted_iota(jnp.int32, (fields, depth), 1)
    stage = [0]

    def set_weights(spacing):
        column = lax.broadcasted_iota(jnp.int32, (fields, 4 * fields), 1)
        row = lax.broadcasted_iota(jnp.int32, (fields, 4 * fields), 0)
        c = damping / (16.0 * spacing)
        square = 12.0 * spacing * spacing
        diff = diff_ref[:, :1]
        diagonal = diff * (-90.0 / square) - 18.0 * c
        m = mix_ref[...]
        m = jnp.where(column < 3 * fields, m * (1.0 / (12.0 * spacing)),
                      m + jnp.where(column - 3 * fields == row, diagonal, 0.0))
        hi = m.astype(bf16).astype(f32)
        lo = m - hi
        for ref, cut in ((weights_x, slice(0, fields)), (weights, slice(fields, 4 * fields))):
            h, l = hi[:, cut], lo[:, cut]
            ref[...] = jnp.concatenate(
                [jnp.concatenate([h, h], axis=1), jnp.concatenate([l, jnp.zeros_like(l)], axis=1)], axis=0).astype(bf16)
        dif = diff_ref[...]
        return dif * (16.0 / square) + 4.0 * c, dif * (-1.0 / square) - c

    def run_stage(section, step, near, far, t, last_store):
        slot = stage[0] % 2
        following = 1 - slot
        copies = halo(slot)
        for copy in copies:
            copy.start()
        if stage[0] > 0:
            for copy in halo(following):
                copy.wait_send()
        def product(stacks, factor):
            wide = jnp.concatenate(stacks, axis=1)
            hi = wide.astype(bf16).astype(f32)
            both = jnp.concatenate([hi, wide - hi], axis=0).astype(bf16)
            got = jnp.dot(factor[...], both, preferred_element_type=f32)
            return got[:fields] + got[fields:]

        def gradient(m2, m1, p1, p2):
            return 8.0 * (p1 - m1) - (p2 - m2)

        def before(y, carry):
            stacks, even = [], []
            for x in range(planes):
                c = u_buf[slot, x, y + 2]
                terms = [tuple(u_buf[slot, x, y + 2 + k] for k in (-2, -1, 1, 2))]
                if t is None:
                    lo2 = lo1 = hi1 = hi2 = c
                else:
                    g = blend(lambda i: gz[i, x, y], t)
                    lo2 = jnp.where(lanes >= depth - 2, g, c)
                    lo1 = jnp.where(lanes == depth - 1, g, c)
                    hi1 = jnp.where(lanes == 0, g, c)
                    hi2 = jnp.where(lanes <= 1, g, c)
                terms.append((pltpu.roll(lo2, 2, 1), pltpu.roll(lo1, 1, 1),
                              pltpu.roll(hi1, depth - 1, 1), pltpu.roll(hi2, depth - 2, 1)))
                stacks.append(jnp.concatenate([gradient(*term) for term in terms] + [c], axis=0))
                even.append(near * sum(m1 + p1 for _, m1, p1, _ in terms) + far * sum(m2 + p2 for m2, _, _, p2 in terms))
            got = product(stacks, weights)
            for x in range(planes):
                part[x, y] = got[:, x * depth:(x + 1) * depth] + even[x]
            return carry

        lax.fori_loop(0, rows, before, 0, unroll=4)
        for copy in copies:
            copy.wait_recv()
        if t is not None:
            for edge, buf in ((0, l_buf), (n - 1, r_buf)):
                @pl.when(me == edge)
                def _(buf=buf):
                    @pl.loop(0, rows)
                    def _(y):
                        for x in range(planes):
                            buf[slot, x, y] = blend(lambda i: gx[i, x, y], t)

        def body(y, carry):
            line = [l_buf[slot, 0, y], l_buf[slot, 1, y], u_buf[slot, 0, y + 2], u_buf[slot, 1, y + 2],
                    r_buf[slot, 0, y], r_buf[slot, 1, y]]
            stacks, even = [], []
            for x in range(planes):
                m2, m1, p1, p2 = line[x], line[x + 1], line[x + 3], line[x + 4]
                stacks.append(gradient(m2, m1, p1, p2))
                even.append(part[x, y] + near * (m1 + p1) + far * (m2 + p2))
            got = product(stacks, weights_x)
            for x in range(planes):
                rate = got[:, x * depth:(x + 1) * depth] + even[x]
                if section == 0:
                    acc[x, y] = start[x, y] + (step / 6.0) * rate
                elif section < 3:
                    acc[x, y] = acc[x, y] + (step / 3.0) * rate
                if section < 3:
                    u_buf[following, x, y + 2] = start[x, y] + (step if section == 2 else 0.5 * step) * rate
                else:
                    last_store(x, y, acc[x, y] + (step / 6.0) * rate, following)
            return carry

        lax.fori_loop(0, rows, body, 0, unroll=4)
        stage[0] += 1

    def wrap_rows():
        slot = stage[0] % 2
        for x in range(planes):
            for k in range(2):
                u_buf[slot, x, k] = u_buf[slot, x, rows + k]
                u_buf[slot, x, rows + 2 + k] = u_buf[slot, x, 2 + k]

    def ghost_rows(t):
        slot = stage[0] % 2
        for x in range(planes):
            for k in range(4):
                row = k if k < 2 else rows + k
                u_buf[slot, x, row] = blend(lambda i: gy[i, x, k], t)

    near, far = set_weights(1.0)

    @pl.loop(0, rows)
    def _(y):
        for x in range(planes):
            start[x, y] = lev_ref[0, x, y]
            u_buf[0, x, y + 2] = lev_ref[0, x, y]

    pack_window(lambda x, y: lev_ref[0, x, y], 0)
    gather_start(gath_old, pay.at[0], 0)
    gath_old[core, pair] = pay[0]

    def coarse_store(x, y, value, following):
        start[x, y] = value

    for section in range(4):
        wrap_rows()
        run_stage(section, coarse_step, near, far, None, coarse_store)
        if section == 0:
            gather_middle(gath_old, pay.at[0], 0)
        elif section == 2:
            gather_last(gath_old, 0)

    pack_window(lambda x, y: start[x, y], 1)
    gather_start(gath_new, pay.at[1], 1)
    gath_new[core, pair] = pay[1]

    near, far = set_weights(0.5)

    @pl.loop(0, rows)
    def _(y):
        for x in range(planes):
            out_ref[0, x, y] = start[x, y]
            start[x, y] = lev_ref[1, x, y]
            u_buf[stage[0] % 2, x, y + 2] = lev_ref[1, x, y]

    gather_end(gath_old, 0)

    def held(t, g, k):
        d = g // planes
        return (gath_old, gath_new)[t][lax.rem(d, 2), d // 2, lax.rem(g, planes), k]

    def window_rows(t, first, w0, w1, which):
        g0 = lax.rem(p + total - 2 + first, total)
        g1 = lax.rem(p + total - 1 + first, total)
        tiles = [w0 * held(t, g0, k) + w1 * held(t, g1, k)
                 for k in range(win_y // 2 + 1)]
        main = split_dot(jnp.concatenate(tiles[:-1], axis=0), exp_ref[...])
        turned = [tiles[-1]] + [pltpu.roll(tiles[-1], depth - 4 * a, 1) for a in range(1, win_y)]
        extra = split_dot(jnp.concatenate(turned, axis=0), expx_ref[...])
        found = []
        for part in which:
            found.append([main[(a // 2) * fields:(a // 2 + 1) * fields,
                               (2 * part + a % 2) * depth:(2 * part + a % 2 + 1) * depth]
                          + extra[a * fields:(a + 1) * fields, part * depth:(part + 1) * depth] for a in range(win_y)])
        return found

    def mix_rows(lines, j):
        low, w0, w1 = hat(j)
        return w0 * lines[low] + w1 * lines[low + 1]

    def ghosts(t):
        for x in range(planes):
            shift, w0, w1 = hat(x + 2)
            inner, outer = window_rows(t, me * (planes // 2) + shift, w0, w1, (0, 1))
            for k in range(4):
                gy[t, x, k] = mix_rows(inner, k if k < 2 else rows + k)
            for y in range(rows):
                gz[t, x, y] = mix_rows(outer, y + 2)
        for edge, base in ((0, 0), (n - 1, total + 2)):
            @pl.when(me == edge)
            def _(base=base):
                for x in range(2):
                    low, w0, w1 = hat(base + x)
                    inner, = window_rows(t, low, w0, w1, (0,))
                    for y in range(rows):
                        gx[t, x, y] = mix_rows(inner, y + 2)

    def fine_store(x, y, value, following):
        start[x, y] = value
        u_buf[following, x, y + 2] = value

    ghosts(0)
    gather_middle(gath_new, pay.at[1], 1)
    for substep in range(2):
        for section in range(4):
            if substep == 0 and section == 1:
                gather_last(gath_new, 1)
                gather_end(gath_new, 1)
                ghosts(1)
            t = 0.5 * (substep + fractions[section])
            ghost_rows(t)
            run_stage(section, 0.5 * coarse_step, near, far, t, fine_store)
    for copy in halo(1 - stage[0] % 2):
        copy.wait_send()

    folded = []
    for y in range(half_y):
        folded.append(start[0, 2 * y] + start[0, 2 * y + 1] + start[1, 2 * y] + start[1, 2 * y + 1])
    got = split_dot(jnp.concatenate(folded, axis=0), mean_ref[...])
    for t in range(half_y // 2):
        sums[t] = (got[2 * t * fields:(2 * t + 1) * fields]
                    + pltpu.roll(got[(2 * t + 1) * fields:(2 * t + 2) * fields], half_z, 1))
    gather_start(landed, sums, 2)
    landed[core, pair] = sums[...]
    gather_middle(landed, sums, 2)

    @pl.loop(0, rows)
    def _(y):
        for x in range(planes):
            out_ref[1, x, y] = start[x, y]

    gather_last(landed, 2)
    gather_end(landed, 2)
    distance = lax.rem(lanes - off_ref[2] + depth, depth)
    for x in range(planes):
        relative = lax.rem(me * planes + x - p + total, total)
        source = lax.rem(relative, half_x)
        for k in range(half_y // 2):
            tile = landed[lax.rem(source, 2), source // 2, k]
            placed = split_dot(tile, place_ref[...])
            for parity in range(2):
                acc[0, 2 * k + parity] = placed[:, parity * depth:(parity + 1) * depth]
        for y in range(rows):
            row = lax.rem(y - q + rows, rows)
            value = acc[0, lax.rem(row, half_y)]
            limit = jnp.where(relative < half_x, jnp.where(row < half_y, half_z, 0), 0)
            out_ref[0, x, y] = jnp.where(distance < limit, value, out_ref[0, x, y])


def hats(fine, window):
    return jnp.maximum(0.0, 1.0 - jnp.abs(0.5 * fine.astype(f32) + 0.75 - window.astype(f32)))


def local(n, levels, region_offset, advect, coupling, diffusion):
    count, fields, planes, rows, depth = levels.shape
    half = depth // 2
    total = planes * n
    win_tiles = (rows // 2 + 4) // 2 + 1
    symmetric = 0.5 * (advect + jnp.swapaxes(advect, 1, 2))
    mixing = jnp.concatenate([symmetric[0], symmetric[1], symmetric[2], coupling], axis=1)
    spread = jnp.broadcast_to(diffusion[:, None], (fields, depth))
    swapped = jnp.transpose(levels, (0, 2, 3, 1, 4))
    r = region_offset[2]
    z = jnp.arange(depth, dtype=jnp.int32)[:, None]
    lane = jnp.arange(depth, dtype=jnp.int32)[None, :]
    zsel = jnp.concatenate([
        (lane < half) & (z == jnp.mod(r - 2 + lane, depth)),
        (lane < 4) & (z == jnp.mod(r - 2 + half + lane, depth))], axis=1).astype(bf16)
    outer = jnp.where(lane >= depth - 2, lane - (depth - 2), depth + 2 + lane)
    has = ((lane >= depth - 2) | (lane < 2)).astype(f32)
    parts = []
    for fine, mask in ((lane + 2, 1.0), (outer, has)):
        parts += [jnp.where(z < half, hats(fine, z), 0.0) * mask, jnp.where(z >= half, hats(fine, z - half), 0.0) * mask]
    expand = jnp.concatenate(parts, axis=1).astype(bf16)
    expandx = jnp.concatenate(
        [jnp.where(z < 4, hats(fine, z + half), 0.0) * mask for fine, mask in ((lane + 2, 1.0), (outer, has))],
        axis=1).astype(bf16)
    mean = ((z // 2 == lane) * 0.125).astype(bf16)
    target = jnp.mod(lane - r, depth)
    place = jnp.concatenate([(z == target) & (target < half), (z == target + half) & (target < half)], axis=1).astype(bf16)
    block = (planes, rows, fields, depth)
    vmem = pl.BlockSpec(memory_space=pltpu.VMEM)
    out = pl.pallas_call(
        lambda *refs: kernel(n, *refs),
        out_shape=jax.ShapeDtypeStruct(swapped.shape, f32),
        in_specs=[pl.BlockSpec(memory_space=pltpu.SMEM)] + [vmem] * 8,
        out_specs=vmem,
        scratch_shapes=[
            pltpu.VMEM((2, planes, rows + 4, fields, depth), f32),
            pltpu.VMEM((2,) + block, f32),
            pltpu.VMEM((2,) + block, f32),
            pltpu.VMEM(block, f32),
            pltpu.VMEM(block, f32),
            pltpu.VMEM(block, f32),
            pltpu.VMEM((2 * fields, 6 * fields), bf16),
            pltpu.VMEM((2 * fields, 2 * fields), bf16),
            pltpu.VMEM((2, planes, win_tiles, fields, depth), f32),
            pltpu.VMEM((2, n // 2, planes, win_tiles, fields, depth), f32),
            pltpu.VMEM((2, n // 2, planes, win_tiles, fields, depth), f32),
            pltpu.VMEM((2, planes, 4, fields, depth), f32),
            pltpu.VMEM((2,) + block, f32),
            pltpu.VMEM((2,) + block, f32),
            pltpu.VMEM((rows // 4, fields, depth), f32),
            pltpu.VMEM((2, n // 2, rows // 4, fields, depth), f32),
            pltpu.SemaphoreType.DMA((2, 2)),
            pltpu.SemaphoreType.DMA((2, 2)),
            pltpu.SemaphoreType.DMA((3, n // 4 + 1)),
            pltpu.SemaphoreType.DMA((3, n // 4 + 1)),
        ],
        compiler_params=pltpu.CompilerParams(
            collective_id=0, has_side_effects=True, vmem_limit_bytes=48 * 1024 * 1024),
    )(region_offset, mixing, spread, swapped, zsel, expand, expandx, mean, place)
    return jnp.transpose(out, (0, 3, 1, 2, 4))


def solution(mesh):
    n = mesh.shape["space"]
    return jax.shard_map(
        lambda *args: local(n, *args),
        mesh=mesh,
        in_specs=(P("runs", None, "space", None, None), P("runs"), P(), P(), P()),
        out_specs=P("runs", None, "space", None, None),
        check_vma=False,
    )
```

```python
import jax
import jax.numpy as jnp
from jax import lax
from jax.experimental import pallas as pl
from jax.experimental.pallas import tpu as pltpu
from jax.sharding import PartitionSpec as P

coarse_step = 0.25
damping = 0.2
fractions = (0.0, 0.5, 0.5, 1.0)
f32, bf16 = jnp.float32, jnp.bfloat16


def split_dot(x, m):
    hi = x.astype(bf16)
    lo = (x - hi.astype(f32)).astype(bf16)
    return jnp.dot(hi, m, preferred_element_type=f32) + jnp.dot(lo, m, preferred_element_type=f32)


def hat(j):
    location = 2 * j + 3
    low = location // 4
    return low, 1.0 - (location % 4) / 4.0, (location % 4) / 4.0


def kernel(n, off_ref, mix_ref, diff_ref, lev_ref, zsel_ref, exp_ref, expx_ref, mean_ref, place_ref, out_ref,
           u_buf, l_buf, r_buf, start, acc, part, weights, weights_x, pay, gath_old, gath_new, gy, gz, gx, sums, landed, fine_in, fine_out,
           halo_send, halo_recv, all_send, all_recv):
    planes, rows, fields, depth = lev_ref.shape[1:]
    total = planes * n
    half_x, half_y, half_z = total // 2, rows // 2, depth // 2
    win_y = half_y + 4
    me = lax.axis_index("space")
    right, left = lax.rem(me + 1, n), lax.rem(me + n - 1, n)
    p, q = off_ref[0], off_ref[1]

    barrier = pltpu.get_barrier_semaphore()

    @pl.loop(1, n)
    def _(k):
        pl.semaphore_signal(barrier, inc=1, device_id={"space": lax.rem(me + k, n)}, device_id_type=pl.DeviceIdType.MESH)

    pl.semaphore_wait(barrier, n - 1)

    def snake(d):
        return d + lax.rem(d // 4, 2) * (2 - 4 * lax.rem(d // 2, 2))

    pos = snake(me)
    turned_row = lax.rem(me // 4, 2) == 1
    straight_row = lax.rem(me // 4, 2) == 0
    level = [0]
    core = lax.rem(me, 2)
    pair = me // 2
    across = me + 2 - 4 * lax.rem(pair, 2)
    groups = n // 4
    first = pair - lax.rem(pair, 2)

    def remote(src, dst, kind, k, target):
        return pltpu.make_async_remote_copy(
            src_ref=src, dst_ref=dst, send_sem=all_send.at[kind, k], recv_sem=all_recv.at[kind, k],
            device_id={"space": target}, device_id_type=pl.DeviceIdType.MESH)

    def gather_start(dst, own, kind):
        remote(own, dst.at[core, pair], kind, 0, across).start()

    def gather_middle(dst, own, kind):
        remote(own, dst.at[core, pair], kind, 0, across).wait()

        @pl.loop(1, groups)
        def _(k):
            block = dst.at[core, pl.ds(first, 2)]
            remote(block, block, kind, k, lax.rem(me + 4 * k, n)).start()

    def gather_last(dst, kind):
        @pl.loop(1, groups)
        def _(k):
            block = dst.at[core, pl.ds(first, 2)]
            remote(block, block, kind, k, lax.rem(me + 4 * k, n)).wait()

        remote(dst.at[core], dst.at[core], kind, groups, me + 1 - 2 * core).start()

    def gather_end(dst, kind):
        remote(dst.at[core], dst.at[core], kind, groups, me + 1 - 2 * core).wait()

    def halo(slot):
        copies = []
        base = slot
        slot = slot + 2 * level[0]
        ends = ((0, right, l_buf), (1, left, r_buf))
        if level[0]:
            ends = ((0, snake(lax.rem(pos + 1, n)), l_buf), (1, snake(lax.rem(pos + n - 1, n)), r_buf))
        for side, target, dst in ends:
            copies.append(pltpu.make_async_remote_copy(
                src_ref=u_buf.at[base, :, pl.ds(2, rows)], dst_ref=dst.at[slot],
                send_sem=halo_send.at[slot, side], recv_sem=halo_recv.at[slot, side],
                device_id={"space": target}, device_id_type=pl.DeviceIdType.MESH))
        return copies

    def pack_window(load, kind):
        for x in range(planes):
            picked = [load(x, lax.rem(q + rows - 2 + a, rows)) for a in range(win_y)]
            got = split_dot(jnp.concatenate(picked, axis=0), zsel_ref[...])
            for t in range(win_y // 2):
                even = got[2 * t * fields:(2 * t + 1) * fields, :depth]
                odd = got[(2 * t + 1) * fields:(2 * t + 2) * fields, :depth]
                pay[kind, x, t] = even + pltpu.roll(odd, half_z, 1)
            extra = got[:fields, depth:]
            for a in range(1, win_y):
                extra = extra + pltpu.roll(got[a * fields:(a + 1) * fields, depth:], 4 * a, 1)
            pay[kind, x, win_y // 2] = extra

    def blend(load, t):
        if t in (0.0, 1.0):
            return load(int(t))
        return (1.0 - t) * load(0) + t * load(1)

    lanes = lax.broadcasted_iota(jnp.int32, (fields, depth), 1)
    stage = [0]

    def set_weights(spacing):
        column = lax.broadcasted_iota(jnp.int32, (fields, 4 * fields), 1)
        row = lax.broadcasted_iota(jnp.int32, (fields, 4 * fields), 0)
        c = damping / (16.0 * spacing)
        square = 12.0 * spacing * spacing
        diff = diff_ref[:, :1]
        diagonal = diff * (-90.0 / square) - 18.0 * c
        m = mix_ref[...]
        m = jnp.where(column < 3 * fields, m * (1.0 / (12.0 * spacing)),
                      m + jnp.where(column - 3 * fields == row, diagonal, 0.0))
        hi = m.astype(bf16).astype(f32)
        lo = m - hi
        for ref, cut in ((weights_x, slice(0, fields)), (weights, slice(fields, 4 * fields))):
            h, l = hi[:, cut], lo[:, cut]
            ref[...] = jnp.concatenate(
                [jnp.concatenate([h, h], axis=1), jnp.concatenate([l, jnp.zeros_like(l)], axis=1)], axis=0).astype(bf16)
        dif = diff_ref[...]
        return dif * (16.0 / square) + 4.0 * c, dif * (-1.0 / square) - c

    def run_stage(section, step, near, far, t, last_store):
        slot = stage[0] % 2
        following = 1 - slot
        copies = halo(slot)
        for copy in copies:
            copy.start()
        if stage[0] not in (0, 4):
            for copy in halo(following):
                copy.wait_send()
        def product(stacks, factor):
            wide = jnp.concatenate(stacks, axis=1)
            hi = wide.astype(bf16).astype(f32)
            both = jnp.concatenate([hi, wide - hi], axis=0).astype(bf16)
            got = jnp.dot(factor[...], both, preferred_element_type=f32)
            return got[:fields] + got[fields:]

        def gradient(m2, m1, p1, p2):
            return 8.0 * (p1 - m1) - (p2 - m2)

        def before(y, carry):
            stacks, even = [], []
            for x in range(planes):
                c = u_buf[slot, x, y + 2]
                terms = [tuple(u_buf[slot, x, y + 2 + k] for k in (-2, -1, 1, 2))]
                if t is None:
                    lo2 = lo1 = hi1 = hi2 = c
                else:
                    g = blend(lambda i: gz[i, x, y], t)
                    lo2 = jnp.where(lanes >= depth - 2, g, c)
                    lo1 = jnp.where(lanes == depth - 1, g, c)
                    hi1 = jnp.where(lanes == 0, g, c)
                    hi2 = jnp.where(lanes <= 1, g, c)
                terms.append((pltpu.roll(lo2, 2, 1), pltpu.roll(lo1, 1, 1),
                              pltpu.roll(hi1, depth - 1, 1), pltpu.roll(hi2, depth - 2, 1)))
                stacks.append(jnp.concatenate([gradient(*term) for term in terms] + [c], axis=0))
                even.append(near * sum(m1 + p1 for _, m1, p1, _ in terms) + far * sum(m2 + p2 for m2, _, _, p2 in terms))
            got = product(stacks, weights)
            for x in range(planes):
                part[x, y] = got[:, x * depth:(x + 1) * depth] + even[x]
            return carry

        lax.fori_loop(0, rows, before, 0, unroll=4)
        for copy in copies:
            copy.wait_recv()
        if t is not None:
            for edge, buf in ((0, l_buf), (n - 1, r_buf)):
                @pl.when(pos == edge)
                def _(buf=buf):
                    @pl.loop(0, rows)
                    def _(y):
                        for x in range(planes):
                            buf[slot + 2, x, y] = blend(lambda i: gx[i, x, y], t)

        def body(y, carry):
            there = slot + 2 * level[0]
            line = [l_buf[there, 0, y], l_buf[there, 1, y], u_buf[slot, 0, y + 2], u_buf[slot, 1, y + 2],
                    r_buf[there, 0, y], r_buf[there, 1, y]]
            stacks, even = [], []
            for x in range(planes):
                m2, m1, p1, p2 = line[x], line[x + 1], line[x + 3], line[x + 4]
                stacks.append(gradient(m2, m1, p1, p2))
                even.append(part[x, y] + near * (m1 + p1) + far * (m2 + p2))
            got = product(stacks, weights_x)
            for x in range(planes):
                rate = got[:, x * depth:(x + 1) * depth] + even[x]
                if section == 0:
                    acc[x, y] = start[x, y] + (step / 6.0) * rate
                elif section < 3:
                    acc[x, y] = acc[x, y] + (step / 3.0) * rate
                if section < 3:
                    u_buf[following, x, y + 2] = start[x, y] + (step if section == 2 else 0.5 * step) * rate
                else:
                    last_store(x, y, acc[x, y] + (step / 6.0) * rate, following)
            return carry

        lax.fori_loop(0, rows, body, 0, unroll=4)
        stage[0] += 1

    def wrap_rows():
        slot = stage[0] % 2
        for x in range(planes):
            for k in range(2):
                u_buf[slot, x, k] = u_buf[slot, x, rows + k]
                u_buf[slot, x, rows + 2 + k] = u_buf[slot, x, 2 + k]

    def ghost_rows(t):
        slot = stage[0] % 2
        for x in range(planes):
            for k in range(4):
                row = k if k < 2 else rows + k
                u_buf[slot, x, row] = blend(lambda i: gy[i, x, k], t)

    @pl.when(turned_row)
    def _():
        remote(lev_ref.at[1], fine_in, 3, 0, across).start()

    @pl.when(straight_row)
    def _():
        @pl.loop(0, rows)
        def _(y):
            for x in range(planes):
                fine_in[x, y] = lev_ref[1, x, y]

    near, far = set_weights(1.0)

    @pl.loop(0, rows)
    def _(y):
        for x in range(planes):
            start[x, y] = lev_ref[0, x, y]
            u_buf[0, x, y + 2] = lev_ref[0, x, y]

    pack_window(lambda x, y: lev_ref[0, x, y], 0)
    gather_start(gath_old, pay.at[0], 0)
    gath_old[core, pair] = pay[0]

    def coarse_store(x, y, value, following):
        start[x, y] = value

    for section in range(4):
        wrap_rows()
        run_stage(section, coarse_step, near, far, None, coarse_store)
        if section == 0:
            gather_middle(gath_old, pay.at[0], 0)
        elif section == 2:
            gather_last(gath_old, 0)

    pack_window(lambda x, y: start[x, y], 1)
    gather_start(gath_new, pay.at[1], 1)
    gath_new[core, pair] = pay[1]

    near, far = set_weights(0.5)
    for copy in halo(1 - stage[0] % 2):
        copy.wait_send()
    level[0] = 1

    @pl.when(turned_row)
    def _():
        remote(lev_ref.at[1], fine_in, 3, 0, across).wait()

    @pl.loop(0, rows)
    def _(y):
        for x in range(planes):
            out_ref[0, x, y] = start[x, y]
            start[x, y] = fine_in[x, y]
            u_buf[stage[0] % 2, x, y + 2] = fine_in[x, y]

    gather_end(gath_old, 0)

    def held(t, g, k):
        d = g // planes
        return (gath_old, gath_new)[t][lax.rem(d, 2), d // 2, lax.rem(g, planes), k]

    def window_rows(t, first, w0, w1, which):
        g0 = lax.rem(p + total - 2 + first, total)
        g1 = lax.rem(p + total - 1 + first, total)
        tiles = [w0 * held(t, g0, k) + w1 * held(t, g1, k)
                 for k in range(win_y // 2 + 1)]
        main = split_dot(jnp.concatenate(tiles[:-1], axis=0), exp_ref[...])
        turned = [tiles[-1]] + [pltpu.roll(tiles[-1], depth - 4 * a, 1) for a in range(1, win_y)]
        extra = split_dot(jnp.concatenate(turned, axis=0), expx_ref[...])
        found = []
        for part in which:
            found.append([main[(a // 2) * fields:(a // 2 + 1) * fields,
                               (2 * part + a % 2) * depth:(2 * part + a % 2 + 1) * depth]
                          + extra[a * fields:(a + 1) * fields, part * depth:(part + 1) * depth] for a in range(win_y)])
        return found

    def mix_rows(lines, j):
        low, w0, w1 = hat(j)
        return w0 * lines[low] + w1 * lines[low + 1]

    def ghosts(t):
        for x in range(planes):
            shift, w0, w1 = hat(x + 2)
            inner, outer = window_rows(t, pos * (planes // 2) + shift, w0, w1, (0, 1))
            for k in range(4):
                gy[t, x, k] = mix_rows(inner, k if k < 2 else rows + k)
            for y in range(rows):
                gz[t, x, y] = mix_rows(outer, y + 2)
        for edge, base in ((0, 0), (n - 1, total + 2)):
            @pl.when(pos == edge)
            def _(base=base):
                for x in range(2):
                    low, w0, w1 = hat(base + x)
                    inner, = window_rows(t, low, w0, w1, (0,))
                    for y in range(rows):
                        gx[t, x, y] = mix_rows(inner, y + 2)

    def fine_store(x, y, value, following):
        start[x, y] = value
        u_buf[following, x, y + 2] = value

    ghosts(0)
    gather_middle(gath_new, pay.at[1], 1)
    for substep in range(2):
        for section in range(4):
            if substep == 0 and section == 1:
                gather_last(gath_new, 1)
                gather_end(gath_new, 1)
                ghosts(1)
            t = 0.5 * (substep + fractions[section])
            ghost_rows(t)
            run_stage(section, 0.5 * coarse_step, near, far, t, fine_store)
    for copy in halo(1 - stage[0] % 2):
        copy.wait_send()

    @pl.when(turned_row)
    def _():
        remote(start, fine_out, 4, 0, across).start()

    folded = []
    for y in range(half_y):
        folded.append(start[0, 2 * y] + start[0, 2 * y + 1] + start[1, 2 * y] + start[1, 2 * y + 1])
    got = split_dot(jnp.concatenate(folded, axis=0), mean_ref[...])
    for t in range(half_y // 2):
        sums[t] = (got[2 * t * fields:(2 * t + 1) * fields]
                    + pltpu.roll(got[(2 * t + 1) * fields:(2 * t + 2) * fields], half_z, 1))
    gather_start(landed, sums, 2)
    landed[core, pair] = sums[...]
    gather_middle(landed, sums, 2)

    gather_last(landed, 2)
    gather_end(landed, 2)
    @pl.when(straight_row)
    def _():
        @pl.loop(0, rows)
        def _(y):
            for x in range(planes):
                out_ref[1, x, y] = start[x, y]

    @pl.when(turned_row)
    def _():
        remote(start, fine_out, 4, 0, across).wait()

        @pl.loop(0, rows)
        def _(y):
            for x in range(planes):
                out_ref[1, x, y] = fine_out[x, y]

    distance = lax.rem(lanes - off_ref[2] + depth, depth)
    for x in range(planes):
        relative = lax.rem(me * planes + x - p + total, total)
        source = snake(lax.rem(relative, half_x))
        for k in range(half_y // 2):
            tile = landed[lax.rem(source, 2), source // 2, k]
            placed = split_dot(tile, place_ref[...])
            for parity in range(2):
                acc[0, 2 * k + parity] = placed[:, parity * depth:(parity + 1) * depth]
        for y in range(rows):
            row = lax.rem(y - q + rows, rows)
            value = acc[0, lax.rem(row, half_y)]
            limit = jnp.where(relative < half_x, jnp.where(row < half_y, half_z, 0), 0)
            out_ref[0, x, y] = jnp.where(distance < limit, value, out_ref[0, x, y])


def hats(fine, window):
    return jnp.maximum(0.0, 1.0 - jnp.abs(0.5 * fine.astype(f32) + 0.75 - window.astype(f32)))


def local(n, levels, region_offset, advect, coupling, diffusion):
    count, fields, planes, rows, depth = levels.shape
    half = depth // 2
    total = planes * n
    win_tiles = (rows // 2 + 4) // 2 + 1
    symmetric = 0.5 * (advect + jnp.swapaxes(advect, 1, 2))
    mixing = jnp.concatenate([symmetric[0], symmetric[1], symmetric[2], coupling], axis=1)
    spread = jnp.broadcast_to(diffusion[:, None], (fields, depth))
    swapped = jnp.transpose(levels, (0, 2, 3, 1, 4))
    r = region_offset[2]
    z = jnp.arange(depth, dtype=jnp.int32)[:, None]
    lane = jnp.arange(depth, dtype=jnp.int32)[None, :]
    zsel = jnp.concatenate([
        (lane < half) & (z == jnp.mod(r - 2 + lane, depth)),
        (lane < 4) & (z == jnp.mod(r - 2 + half + lane, depth))], axis=1).astype(bf16)
    outer = jnp.where(lane >= depth - 2, lane - (depth - 2), depth + 2 + lane)
    has = ((lane >= depth - 2) | (lane < 2)).astype(f32)
    parts = []
    for fine, mask in ((lane + 2, 1.0), (outer, has)):
        parts += [jnp.where(z < half, hats(fine, z), 0.0) * mask, jnp.where(z >= half, hats(fine, z - half), 0.0) * mask]
    expand = jnp.concatenate(parts, axis=1).astype(bf16)
    expandx = jnp.concatenate(
        [jnp.where(z < 4, hats(fine, z + half), 0.0) * mask for fine, mask in ((lane + 2, 1.0), (outer, has))],
        axis=1).astype(bf16)
    mean = ((z // 2 == lane) * 0.125).astype(bf16)
    target = jnp.mod(lane - r, depth)
    place = jnp.concatenate([(z == target) & (target < half), (z == target + half) & (target < half)], axis=1).astype(bf16)
    block = (planes, rows, fields, depth)
    vmem = pl.BlockSpec(memory_space=pltpu.VMEM)
    out = pl.pallas_call(
        lambda *refs: kernel(n, *refs),
        out_shape=jax.ShapeDtypeStruct(swapped.shape, f32),
        in_specs=[pl.BlockSpec(memory_space=pltpu.SMEM)] + [vmem] * 8,
        out_specs=vmem,
        scratch_shapes=[
            pltpu.VMEM((2, planes, rows + 4, fields, depth), f32),
            pltpu.VMEM((4,) + block, f32),
            pltpu.VMEM((4,) + block, f32),
            pltpu.VMEM(block, f32),
            pltpu.VMEM(block, f32),
            pltpu.VMEM(block, f32),
            pltpu.VMEM((2 * fields, 6 * fields), bf16),
            pltpu.VMEM((2 * fields, 2 * fields), bf16),
            pltpu.VMEM((2, planes, win_tiles, fields, depth), f32),
            pltpu.VMEM((2, n // 2, planes, win_tiles, fields, depth), f32),
            pltpu.VMEM((2, n // 2, planes, win_tiles, fields, depth), f32),
            pltpu.VMEM((2, planes, 4, fields, depth), f32),
            pltpu.VMEM((2,) + block, f32),
            pltpu.VMEM((2,) + block, f32),
            pltpu.VMEM((rows // 4, fields, depth), f32),
            pltpu.VMEM((2, n // 2, rows // 4, fields, depth), f32),
            pltpu.VMEM(block, f32),
            pltpu.VMEM(block, f32),
            pltpu.SemaphoreType.DMA((4, 2)),
            pltpu.SemaphoreType.DMA((4, 2)),
            pltpu.SemaphoreType.DMA((5, n // 4 + 1)),
            pltpu.SemaphoreType.DMA((5, n // 4 + 1)),
        ],
        compiler_params=pltpu.CompilerParams(
            collective_id=0, has_side_effects=True, vmem_limit_bytes=48 * 1024 * 1024),
    )(region_offset, mixing, spread, swapped, zsel, expand, expandx, mean, place)
    return jnp.transpose(out, (0, 3, 1, 2, 4))


def solution(mesh):
    n = mesh.shape["space"]
    return jax.shard_map(
        lambda *args: local(n, *args),
        mesh=mesh,
        in_specs=(P("runs", None, "space", None, None), P("runs"), P(), P(), P()),
        out_specs=P("runs", None, "space", None, None),
        check_vma=False,
    )
```
